8 devices in a mesh: dp: 1 (over z), tp: 8 (over y, x, core).
Axes of the slice: x: 2, y: 2, z: 1, core: 2. Of those that a mesh axis runs over, the one named last changes fastest.
Arguments:
- x_chunk: bfloat16 [8, 512, 4096], P('dp', 'tp')
- prefix_len: int32 [8], P('dp')
- k_cache: bfloat16 [8, 4096, 32, 128], P('dp', None, 'tp')
- v_cache: bfloat16 [8, 4096, 32, 128], P('dp', None, 'tp')
- ln1_gain: bfloat16 [4096], replicated
- ln1_bias: bfloat16 [4096], replicated
- w_qkv: bfloat16 [4096, 12288], P(None, 'tp')
- b_qkv: bfloat16 [12288], P('tp')
- w_out: bfloat16 [4096, 4096], P('tp')
- b_out: bfloat16 [4096], replicated
- ln2_gain: bfloat16 [4096], replicated
- ln2_bias: bfloat16 [4096], replicated
- w_up: bfloat16 [4096, 16384], P(None, 'tp')
- b_up: bfloat16 [16384], P('tp')
- w_down: bfloat16 [16384, 4096], P('tp')
- b_down: bfloat16 [4096], replicated
Outputs:
- output 1: bfloat16 [8, 512, 4096], P('dp', 'tp')
- output 2: bfloat16 [8, 4096, 32, 128], P('dp', None, 'tp')
- output 3: bfloat16 [8, 4096, 32, 128], P('dp', None, 'tp')
All inputs are finite; a program needn't handle non-finite values.
Results may differ from the reference program's by a relative error of at most 0.0125854.
Values are sent between devices in bfloat16 or wider.
A program may use at most 1 GiB of HBM per device.

```python
import jax
import jax.numpy as jnp
from jax import lax

BATCH_SEQS = 8
CHUNK_LEN = 512
CACHE_LEN = 4096
D_MODEL = 4096
NUM_HEADS = 32
HEAD_DIM = 128
FF_DIM = 4 * D_MODEL
LN_EPS = 1e-5


def setup_inputs(seed: int = 0, part: int = 0) -> dict:
    part_keys = jax.random.split(jax.random.fold_in(jax.random.key(seed), part), 5)
    shared_keys = jax.random.split(jax.random.key(seed + 7919), 12)
    max_start = CACHE_LEN - CHUNK_LEN
    starts = jax.random.randint(part_keys[1], (BATCH_SEQS,), 0, max_start + 1)
    longest = jax.random.randint(part_keys[2], (), 0, BATCH_SEQS)
    prefix_len = jnp.where(jnp.arange(BATCH_SEQS) == longest, max_start, starts).astype(jnp.int32)
    cache_shape = (BATCH_SEQS, CACHE_LEN, NUM_HEADS, HEAD_DIM)
    vec_shape = (D_MODEL,)
    d_scale = D_MODEL ** -0.5

    def normal_draw(key_in, shape_in, std_dev):
        return (std_dev * jax.random.normal(key_in, shape_in, jnp.float32)).astype(jnp.bfloat16)

    def gain_draw(key_in):
        return (1.0 + 0.25 * jax.random.normal(key_in, vec_shape, jnp.float32)).astype(jnp.bfloat16)

    return {
        'x_chunk': normal_draw(part_keys[0], (BATCH_SEQS, CHUNK_LEN, D_MODEL), 1.0),
        'prefix_len': prefix_len,
        'k_cache': normal_draw(part_keys[3], cache_shape, 1.0),
        'v_cache': normal_draw(part_keys[4], cache_shape, 1.0),
        'ln1_gain': gain_draw(shared_keys[0]),
        'ln1_bias': normal_draw(shared_keys[1], vec_shape, 0.25),
        'w_qkv': normal_draw(shared_keys[2], (D_MODEL, 3 * D_MODEL), d_scale),
        'b_qkv': normal_draw(shared_keys[3], (3 * D_MODEL,), 0.25),
        'w_out': normal_draw(shared_keys[4], (D_MODEL, D_MODEL), d_scale),
        'b_out': normal_draw(shared_keys[5], vec_shape, 0.25),
        'ln2_gain': gain_draw(shared_keys[6]),
        'ln2_bias': normal_draw(shared_keys[7], vec_shape, 0.25),
        'w_up': normal_draw(shared_keys[8], (D_MODEL, FF_DIM), d_scale),
        'b_up': normal_draw(shared_keys[9], (FF_DIM,), 0.25),
        'w_down': normal_draw(shared_keys[10], (FF_DIM, D_MODEL), FF_DIM ** -0.5),
        'b_down': normal_draw(shared_keys[11], vec_shape, 0.25),
    }


def layer_norm(tok_rows, ln_gain, ln_bias):
    rows_f32 = tok_rows.astype(jnp.float32)
    row_mean = jnp.mean(rows_f32, axis=-1, keepdims=True)
    centered = rows_f32 - row_mean
    row_var = jnp.mean(centered * centered, axis=-1, keepdims=True)
    normed = centered * lax.rsqrt(row_var + LN_EPS)
    return (normed * ln_gain.astype(jnp.float32) + ln_bias.astype(jnp.float32)).astype(jnp.bfloat16)


def write_rows(cache_seq, new_rows, start_pos):
    zero_idx = jnp.zeros_like(start_pos)
    return lax.dynamic_update_slice(cache_seq, new_rows, (start_pos, zero_idx, zero_idx))


def attend_one(operands):
    queries, keys_all, values_all, start_pos = operands
    scores = jnp.einsum('chd,thd->hct', queries.astype(jnp.float32), keys_all.astype(jnp.float32)) * (HEAD_DIM ** -0.5)
    slopes = jnp.exp2(-8.0 * (jnp.arange(NUM_HEADS) + 1).astype(jnp.float32) / NUM_HEADS)
    query_pos = start_pos + jnp.arange(CHUNK_LEN)
    rel_pos = (jnp.arange(CACHE_LEN)[None, :] - query_pos[:, None]).astype(jnp.float32)
    scores = scores + slopes[:, None, None] * rel_pos[None]
    scores = jnp.where((rel_pos <= 0.0)[None], scores, -1e30)
    attn_probs = jax.nn.softmax(scores, axis=-1).astype(jnp.bfloat16)
    context = jnp.einsum('hct,thd->chd', attn_probs.astype(jnp.float32), values_all.astype(jnp.float32))
    return context.astype(jnp.bfloat16).reshape(CHUNK_LEN, D_MODEL)


def reference(x_chunk, prefix_len, k_cache, v_cache, ln1_gain, ln1_bias, w_qkv, b_qkv, w_out, b_out, ln2_gain, ln2_bias, w_up, b_up, w_down, b_down):
    tok_rows = x_chunk.reshape(BATCH_SEQS * CHUNK_LEN, D_MODEL)
    normed = layer_norm(tok_rows, ln1_gain, ln1_bias)
    qkv_proj = jnp.dot(normed, w_qkv, preferred_element_type=jnp.float32) + b_qkv.astype(jnp.float32)
    qkv_heads = qkv_proj.astype(jnp.bfloat16).reshape(BATCH_SEQS, CHUNK_LEN, NUM_HEADS, 3, HEAD_DIM)
    k_upd = jax.vmap(write_rows)(k_cache, qkv_heads[:, :, :, 1], prefix_len)
    v_upd = jax.vmap(write_rows)(v_cache, qkv_heads[:, :, :, 2], prefix_len)
    context = lax.map(attend_one, (qkv_heads[:, :, :, 0], k_upd, v_upd, prefix_len))
    context = context.reshape(BATCH_SEQS * CHUNK_LEN, D_MODEL)
    attn_out = jnp.dot(context, w_out, preferred_element_type=jnp.float32)
    residual = (tok_rows.astype(jnp.float32) + attn_out + b_out.astype(jnp.float32)).astype(jnp.bfloat16)
    normed2 = layer_norm(residual, ln2_gain, ln2_bias)
    up_pre = jnp.dot(normed2, w_up, preferred_element_type=jnp.float32) + b_up.astype(jnp.float32)
    up_act = jax.nn.gelu(up_pre, approximate=True).astype(jnp.bfloat16)
    down_out = jnp.dot(up_act, w_down, preferred_element_type=jnp.float32)
    x_out = (residual.astype(jnp.float32) + down_out + b_down.astype(jnp.float32)).astype(jnp.bfloat16)
    return x_out.reshape(BATCH_SEQS, CHUNK_LEN, D_MODEL), k_upd, v_upd
```

```python
import functools

import jax
import jax.numpy as jnp
from jax import lax
from jax.experimental import pallas as pl
from jax.experimental.pallas import tpu as pltpu
from jax.sharding import PartitionSpec as P

LN_EPS = 1e-5
LOG2E = 1.4426950408889634
N_CHUNKS = 4
KV_BLOCK = 512
PAIR_FIRST = True


def norm_rows(rows_f32, gain_ref, bias_ref):
    row_mean = jnp.mean(rows_f32, axis=-1, keepdims=True)
    centered = rows_f32 - row_mean
    row_var = jnp.mean(centered * centered, axis=-1, keepdims=True)
    normed = centered * lax.rsqrt(row_var + LN_EPS)
    return (normed * gain_ref[...].astype(jnp.float32) + bias_ref[...].astype(jnp.float32)).astype(jnp.bfloat16)


def norm_kernel(x_ref, gain_ref, bias_ref, out_ref):
    out_ref[0] = norm_rows(x_ref[0].astype(jnp.float32), gain_ref, bias_ref)


def add_norm_kernel(x_ref, sum_ref, b_ref, gain_ref, bias_ref, res_ref, out_ref):
    res = (x_ref[0].astype(jnp.float32) + sum_ref[0].astype(jnp.float32) + b_ref[...].astype(jnp.float32)).astype(jnp.bfloat16)
    res_ref[0] = res
    out_ref[0] = norm_rows(res.astype(jnp.float32), gain_ref, bias_ref)


def add_kernel(x_ref, sum_ref, b_ref, *refs):
    refs[-1][0] = (x_ref[0].astype(jnp.float32) + sum_ref[0].astype(jnp.float32) + b_ref[...].astype(jnp.float32)).astype(jnp.bfloat16)


def copy_kernel(after_ref, k_ref, v_ref, k_out, v_out):
    k_out[...] = k_ref[...]
    v_out[...] = v_ref[...]


def copy_caches(k_rows, v_rows, after):
    batch_n, rows, head_dim = k_rows.shape
    block = min(4096, rows)
    spec = pl.BlockSpec((1, block, head_dim), lambda b, i: (b, i, 0))
    shape = jax.ShapeDtypeStruct(k_rows.shape, k_rows.dtype)
    return pl.pallas_call(
        copy_kernel, grid=(batch_n, rows // block), in_specs=[pl.BlockSpec(memory_space=pl.ANY), spec, spec], out_specs=[spec, spec],
        out_shape=[shape, shape], name="copy_caches",
        cost_estimate=pl.CostEstimate(flops=k_rows.size * 4, bytes_accessed=k_rows.size * 8, transcendentals=0),
    )(after, k_rows, v_rows)


def row_specs(first_seq, tok_loc, d_model):
    whole = pl.BlockSpec((1, tok_loc, d_model), lambda i: (first_seq + i, 0, 0))
    own = pl.BlockSpec((1, tok_loc, d_model), lambda i: (i, 0, 0))
    vec = pl.BlockSpec((1, d_model), lambda i: (0, 0))
    return whole, own, vec


def norm_chunk(x_local, gain, bias, first_seq, seqs):
    _, tok_loc, d_model = x_local.shape
    whole, own, vec = row_specs(first_seq, tok_loc, d_model)
    size = seqs * tok_loc * d_model
    return pl.pallas_call(
        norm_kernel, grid=(seqs,), in_specs=[whole, vec, vec], out_specs=own,
        out_shape=jax.ShapeDtypeStruct((seqs, tok_loc, d_model), jnp.bfloat16),
        cost_estimate=pl.CostEstimate(flops=size * 20, bytes_accessed=size * 4, transcendentals=0), name="norm_in",
    )(x_local, gain, bias)


def add_norm_chunk(x_local, summed, b, gain, bias, first_seq, seqs):
    _, tok_loc, d_model = x_local.shape
    whole, own, vec = row_specs(first_seq, tok_loc, d_model)
    size = seqs * tok_loc * d_model
    shape = jax.ShapeDtypeStruct((seqs, tok_loc, d_model), jnp.bfloat16)
    return pl.pallas_call(
        add_norm_kernel, grid=(seqs,), in_specs=[whole, own, vec, vec, vec], out_specs=[own, own], out_shape=[shape, shape],
        cost_estimate=pl.CostEstimate(flops=size * 24, bytes_accessed=size * 8, transcendentals=0), name="add_norm",
    )(x_local, summed, b, gain, bias)


def add_chunk(res, summed, b, prev, first_seq, batch_n):
    seqs, tok_loc, d_model = res.shape
    whole, own, vec = row_specs(first_seq, tok_loc, d_model)
    size = seqs * tok_loc * d_model
    args, specs, aliases = [res, summed, b], [own, own, vec], {}
    if prev is not None:
        args.append(prev)
        specs.append(pl.BlockSpec(memory_space=pl.ANY))
        aliases = {3: 0}
    return pl.pallas_call(
        add_kernel, grid=(seqs,), in_specs=specs, out_specs=whole, input_output_aliases=aliases,
        out_shape=jax.ShapeDtypeStruct((batch_n, tok_loc, d_model), jnp.bfloat16),
        cost_estimate=pl.CostEstimate(flops=size * 4, bytes_accessed=size * 6, transcendentals=0), name="add_out",
    )(*args)


def attn_kernel(heads_loc, head_dim, block, first_seq, len_ref, slope_ref, qkv_ref, k_ref, v_ref, ctx_ref, kn_ref, vn_ref, k32, v32, m_s, l_s, acc_s):
    step = pl.program_id(1)
    start = len_ref[first_seq + pl.program_id(0)]
    chunk = qkv_ref.shape[1]
    scale = head_dim ** -0.5 * LOG2E
    contract_last = (((1,), (1,)), ((), ()))
    contract = (((1,), (0,)), ((), ()))

    @pl.when(step == 0)
    def _():
        row = lax.broadcasted_iota(jnp.int32, (chunk, chunk), 0)
        col = lax.broadcasted_iota(jnp.int32, (chunk, chunk), 1)
        col_f = lax.broadcasted_iota(jnp.int32, (1, chunk), 1).astype(jnp.float32)

        def head(h, carry):
            base = pl.multiple_of(h * (3 * head_dim), head_dim)
            q = qkv_ref[0, :, pl.ds(base, head_dim)]
            k = qkv_ref[0, :, pl.ds(base + head_dim, head_dim)]
            v = qkv_ref[0, :, pl.ds(base + 2 * head_dim, head_dim)]
            k32[pl.ds(h, chunk, stride=heads_loc), :] = k.astype(jnp.float32)
            v32[pl.ds(h, chunk, stride=heads_loc), :] = v.astype(jnp.float32)
            s = lax.dot_general(q, k, contract_last, preferred_element_type=jnp.float32) * scale
            s = s + slope_ref[h] * col_f
            s = jnp.where(col <= row, s, -1e30)
            m = jnp.max(s, axis=1, keepdims=True)
            p = jnp.exp2(s - m)
            m_s[h] = jnp.broadcast_to(m, (chunk, head_dim))
            l_s[h] = jnp.broadcast_to(jnp.sum(p, axis=1, keepdims=True), (chunk, head_dim))
            acc_s[h] = lax.dot_general(p.astype(jnp.bfloat16), v, contract, preferred_element_type=jnp.float32)
            return carry

        lax.fori_loop(0, heads_loc, head, 0)
        kn_ref[0] = k32[...].astype(jnp.bfloat16)
        vn_ref[0] = v32[...].astype(jnp.bfloat16)

    first = (step - 1) * block

    @pl.when((step > 0) & (first < start))
    def _():
        k32[...] = k_ref[0].astype(jnp.float32)
        v32[...] = v_ref[0].astype(jnp.float32)
        pos_col = first + lax.broadcasted_iota(jnp.int32, (block, head_dim), 0)
        pos = first + lax.broadcasted_iota(jnp.int32, (1, block), 1)
        rel = (pos - start).astype(jnp.float32)

        def head(h, carry):
            base = pl.multiple_of(h * (3 * head_dim), head_dim)
            q = qkv_ref[0, :, pl.ds(base, head_dim)]
            k = k32[pl.ds(h, block, stride=heads_loc), :]
            k = jnp.where(pos_col < start, k, 0.0).astype(jnp.bfloat16)
            v = v32[pl.ds(h, block, stride=heads_loc), :].astype(jnp.bfloat16)
            bias = jnp.where(pos < start, slope_ref[h] * rel, -1e30)
            s = lax.dot_general(q, k, contract_last, preferred_element_type=jnp.float32) * scale + bias
            m_old = m_s[h]
            m_new = jnp.maximum(m_old, jnp.max(s, axis=1, keepdims=True))
            p = jnp.exp2(s - jnp.tile(m_new, (1, block // head_dim)))
            alpha = jnp.exp2(m_old - m_new)
            m_s[h] = m_new
            l_s[h] = l_s[h] * alpha + jnp.sum(p, axis=1, keepdims=True)
            acc_s[h] = acc_s[h] * alpha + lax.dot_general(p.astype(jnp.bfloat16), v, contract, preferred_element_type=jnp.float32)
            return carry

        lax.fori_loop(0, heads_loc, head, 0)

    @pl.when(step == pl.num_programs(1) - 1)
    def _():
        for h in range(heads_loc):
            ctx_ref[0, :, h * head_dim:(h + 1) * head_dim] = (acc_s[h] / l_s[h]).astype(jnp.bfloat16)


def attention(qkv, k_rows, v_rows, prefix_len, slopes, first_seq, heads_loc, head_dim, cache_len):
    seqs, chunk, width = qkv.shape
    block = KV_BLOCK
    blocks = pl.cdiv(cache_len - chunk, block)

    def kv_map(b, j, lens, sl):
        last = jnp.maximum((lens[first_seq + b] + block - 1) // block - 1, 0)
        return (first_seq + b, jnp.clip(j - 1, 0, last), 0)

    kv_spec = pl.BlockSpec((1, block * heads_loc, head_dim), kv_map)
    new_spec = pl.BlockSpec((1, chunk * heads_loc, head_dim), lambda b, j, lens, sl: (b, 0, 0))
    rows_max = max(block, chunk) * heads_loc
    macs = 2 * seqs * chunk * cache_len * heads_loc * head_dim
    return pl.pallas_call(
        functools.partial(attn_kernel, heads_loc, head_dim, block, first_seq),
        grid_spec=pltpu.PrefetchScalarGridSpec(
            num_scalar_prefetch=2,
            grid=(seqs, blocks + 1),
            in_specs=[pl.BlockSpec((1, chunk, width), lambda b, j, lens, sl: (b, 0, 0)), kv_spec, kv_spec],
            out_specs=[pl.BlockSpec((1, chunk, heads_loc * head_dim), lambda b, j, lens, sl: (b, 0, 0)), new_spec, new_spec],
            scratch_shapes=[
                pltpu.VMEM((rows_max, head_dim), jnp.float32),
                pltpu.VMEM((rows_max, head_dim), jnp.float32),
                pltpu.VMEM((heads_loc, chunk, head_dim), jnp.float32),
                pltpu.VMEM((heads_loc, chunk, head_dim), jnp.float32),
                pltpu.VMEM((heads_loc, chunk, head_dim), jnp.float32),
            ],
        ),
        out_shape=[
            jax.ShapeDtypeStruct((seqs, chunk, heads_loc * head_dim), jnp.bfloat16),
            jax.ShapeDtypeStruct((seqs, chunk * heads_loc, head_dim), jnp.bfloat16),
            jax.ShapeDtypeStruct((seqs, chunk * heads_loc, head_dim), jnp.bfloat16),
        ],
        compiler_params=pltpu.CompilerParams(dimension_semantics=("arbitrary", "arbitrary")),
        cost_estimate=pl.CostEstimate(flops=2 * macs, bytes_accessed=4 * seqs * cache_len * heads_loc * head_dim, transcendentals=0),
        name="prefill_attention",
    )(prefix_len, slopes, qkv, k_rows, v_rows)


def solution(mesh):
    tp_size = mesh.shape['tp']

    def local_layer(x_local, prefix_len, k_cache, v_cache, ln1_gain, ln1_bias, w_qkv, b_qkv, w_out, b_out, ln2_gain, ln2_bias, w_up, b_up, w_down, b_down):
        batch_n, tok_loc, d_model = x_local.shape
        cache_len, heads_loc, head_dim = k_cache.shape[1:]
        chunk_len = tok_loc * tp_size
        head_ids = lax.axis_index('tp') * heads_loc + jnp.arange(heads_loc)
        slopes = jnp.exp2(-8.0 * (head_ids + 1).astype(jnp.float32) / (heads_loc * tp_size)) * LOG2E
        k_rows = k_cache.reshape(batch_n, cache_len * heads_loc, head_dim)
        v_rows = v_cache.reshape(batch_n, cache_len * heads_loc, head_dim)
        seqs = batch_n // N_CHUNKS
        core = lax.axis_index('tp') % 2
        pairs = [(i, i ^ 1) for i in range(tp_size)]
        same_core = [[i for i in range(tp_size) if i % 2 == c] for c in range(2)]
        vecs = [v.reshape(1, d_model) for v in (ln1_gain, ln1_bias, b_out, ln2_gain, ln2_bias, b_down)]
        gain1, bias1, bias_out, gain2, bias2, bias_down = vecs

        def gather(rows):
            return lax.all_gather(rows, 'tp', axis=1, tiled=True)

        def reduce_scatter(acts, weights):
            if not PAIR_FIRST:
                part = jnp.einsum('bce,ed->bcd', acts, weights, preferred_element_type=jnp.float32).astype(jnp.bfloat16)
                return lax.psum_scatter(part, 'tp', scatter_dimension=1, tiled=True)
            by_core = acts.reshape(seqs, tp_size // 2, 2, tok_loc, acts.shape[-1])

            def half(which):
                mine = lax.dynamic_index_in_dim(by_core, which, axis=2, keepdims=False).reshape(seqs, chunk_len // 2, acts.shape[-1])
                return jnp.einsum('bce,ed->bcd', mine, weights, preferred_element_type=jnp.float32)

            other = lax.ppermute(half(1 - core).astype(jnp.bfloat16), 'tp', pairs)
            part = (half(core) + other.astype(jnp.float32)).astype(jnp.bfloat16)
            return lax.psum_scatter(part, 'tp', scatter_dimension=1, tiled=True, axis_index_groups=same_core)

        normed = [norm_chunk(x_local, gain1, bias1, c * seqs, seqs) for c in range(N_CHUNKS)]
        k_upd, v_upd = (rows.reshape(k_cache.shape) for rows in copy_caches(k_rows, v_rows, normed[-1]))
        gathered = [gather(rows) for rows in normed]
        contexts = []
        for c in range(N_CHUNKS):
            qkv = (jnp.einsum('bcd,de->bce', gathered[c], w_qkv, preferred_element_type=jnp.float32) + b_qkv.astype(jnp.float32)).astype(jnp.bfloat16)
            context, k_new, v_new = attention(qkv, k_rows, v_rows, prefix_len, slopes, c * seqs, heads_loc, head_dim, cache_len)
            contexts.append(context)
            k_new = k_new.reshape(seqs, chunk_len, heads_loc, head_dim)
            v_new = v_new.reshape(seqs, chunk_len, heads_loc, head_dim)
            for b in range(seqs):
                at = (c * seqs + b, prefix_len[c * seqs + b], 0, 0)
                k_upd = lax.dynamic_update_slice(k_upd, k_new[b:b + 1], at)
                v_upd = lax.dynamic_update_slice(v_upd, v_new[b:b + 1], at)
        x_out = None
        for c in range(N_CHUNKS):
            attn_sum = reduce_scatter(contexts[c], w_out)
            residual, normed2 = add_norm_chunk(x_local, attn_sum, bias_out, gain2, bias2, c * seqs, seqs)
            up_pre = jnp.einsum('bcd,df->bcf', gather(normed2), w_up, preferred_element_type=jnp.float32) + b_up.astype(jnp.float32)
            up_act = jax.nn.gelu(up_pre, approximate=True).astype(jnp.bfloat16)
            x_out = add_chunk(residual, reduce_scatter(up_act, w_down), bias_down, x_out, c * seqs, batch_n)
        return x_out, k_upd, v_upd

    tok_spec = P('dp', 'tp', None)
    cache_spec = P('dp', None, 'tp', None)
    replicated = P()
    in_specs = (tok_spec, P('dp'), cache_spec, cache_spec, replicated, replicated, P(None, 'tp'), P('tp'), P('tp', None), replicated, replicated, replicated, P(None, 'tp'), P('tp'), P('tp', None), replicated)
    return jax.shard_map(local_layer, mesh=mesh, in_specs=in_specs, out_specs=(tok_spec, cache_spec, cache_spec), check_vma=False)
```

```python
import functools

import jax
import jax.numpy as jnp
from jax import lax
from jax.experimental import pallas as pl
from jax.experimental.pallas import tpu as pltpu
from jax.sharding import PartitionSpec as P

LN_EPS = 1e-5
LOG2E = 1.4426950408889634
N_CHUNKS = 4
MLP_GROUPS = 2
KV_BLOCK = 512
PAIR_FIRST = True


def norm_rows(rows_f32, gain_ref, bias_ref):
    row_mean = jnp.mean(rows_f32, axis=-1, keepdims=True)
    centered = rows_f32 - row_mean
    row_var = jnp.mean(centered * centered, axis=-1, keepdims=True)
    normed = centered * lax.rsqrt(row_var + LN_EPS)
    return (normed * gain_ref[...].astype(jnp.float32) + bias_ref[...].astype(jnp.float32)).astype(jnp.bfloat16)


def norm_kernel(x_ref, gain_ref, bias_ref, out_ref):
    out_ref[0] = norm_rows(x_ref[0].astype(jnp.float32), gain_ref, bias_ref)


def add_norm_kernel(x_ref, sum_ref, b_ref, gain_ref, bias_ref, res_ref, out_ref):
    res = (x_ref[0].astype(jnp.float32) + sum_ref[0].astype(jnp.float32) + b_ref[...].astype(jnp.float32)).astype(jnp.bfloat16)
    res_ref[0] = res
    out_ref[0] = norm_rows(res.astype(jnp.float32), gain_ref, bias_ref)


def add_kernel(x_ref, sum_ref, b_ref, *refs):
    refs[-1][0] = (x_ref[0].astype(jnp.float32) + sum_ref[0].astype(jnp.float32) + b_ref[...].astype(jnp.float32)).astype(jnp.bfloat16)


def copy_kernel(after_ref, k_ref, v_ref, k_out, v_out):
    k_out[...] = k_ref[...]
    v_out[...] = v_ref[...]


def copy_caches(k_rows, v_rows, after):
    batch_n, rows, head_dim = k_rows.shape
    block = min(4096, rows)
    spec = pl.BlockSpec((1, block, head_dim), lambda b, i: (b, i, 0))
    shape = jax.ShapeDtypeStruct(k_rows.shape, k_rows.dtype)
    return pl.pallas_call(
        copy_kernel, grid=(batch_n, rows // block), in_specs=[pl.BlockSpec(memory_space=pl.ANY), spec, spec], out_specs=[spec, spec],
        out_shape=[shape, shape], name="copy_caches",
        cost_estimate=pl.CostEstimate(flops=k_rows.size * 4, bytes_accessed=k_rows.size * 8, transcendentals=0),
    )(after, k_rows, v_rows)


def row_specs(first_seq, tok_loc, d_model):
    whole = pl.BlockSpec((1, tok_loc, d_model), lambda i: (first_seq + i, 0, 0))
    own = pl.BlockSpec((1, tok_loc, d_model), lambda i: (i, 0, 0))
    vec = pl.BlockSpec((1, d_model), lambda i: (0, 0))
    return whole, own, vec


def norm_chunk(x_local, gain, bias, first_seq, seqs):
    _, tok_loc, d_model = x_local.shape
    whole, own, vec = row_specs(first_seq, tok_loc, d_model)
    size = seqs * tok_loc * d_model
    return pl.pallas_call(
        norm_kernel, grid=(seqs,), in_specs=[whole, vec, vec], out_specs=own,
        out_shape=jax.ShapeDtypeStruct((seqs, tok_loc, d_model), jnp.bfloat16),
        cost_estimate=pl.CostEstimate(flops=size * 20, bytes_accessed=size * 4, transcendentals=0), name="norm_in",
    )(x_local, gain, bias)


def add_norm_chunk(x_local, summed, b, gain, bias, first_seq, seqs):
    _, tok_loc, d_model = x_local.shape
    whole, own, vec = row_specs(first_seq, tok_loc, d_model)
    size = seqs * tok_loc * d_model
    shape = jax.ShapeDtypeStruct((seqs, tok_loc, d_model), jnp.bfloat16)
    return pl.pallas_call(
        add_norm_kernel, grid=(seqs,), in_specs=[whole, own, vec, vec, vec], out_specs=[own, own], out_shape=[shape, shape],
        cost_estimate=pl.CostEstimate(flops=size * 24, bytes_accessed=size * 8, transcendentals=0), name="add_norm",
    )(x_local, summed, b, gain, bias)


def add_chunk(res, summed, b, prev, first_seq, batch_n):
    seqs, tok_loc, d_model = res.shape
    whole, own, vec = row_specs(first_seq, tok_loc, d_model)
    size = seqs * tok_loc * d_model
    args, specs, aliases = [res, summed, b], [own, own, vec], {}
    if prev is not None:
        args.append(prev)
        specs.append(pl.BlockSpec(memory_space=pl.ANY))
        aliases = {3: 0}
    return pl.pallas_call(
        add_kernel, grid=(seqs,), in_specs=specs, out_specs=whole, input_output_aliases=aliases,
        out_shape=jax.ShapeDtypeStruct((batch_n, tok_loc, d_model), jnp.bfloat16),
        cost_estimate=pl.CostEstimate(flops=size * 4, bytes_accessed=size * 6, transcendentals=0), name="add_out",
    )(*args)


def attn_kernel(heads_loc, head_dim, block, first_seq, len_ref, slope_ref, qkv_ref, k_ref, v_ref, ctx_ref, kn_ref, vn_ref, k32, v32, m_s, l_s, acc_s):
    step = pl.program_id(1)
    start = len_ref[first_seq + pl.program_id(0)]
    chunk = qkv_ref.shape[1]
    scale = head_dim ** -0.5 * LOG2E
    contract_last = (((1,), (1,)), ((), ()))
    contract = (((1,), (0,)), ((), ()))

    @pl.when(step == 0)
    def _():
        row = lax.broadcasted_iota(jnp.int32, (chunk, chunk), 0)
        col = lax.broadcasted_iota(jnp.int32, (chunk, chunk), 1)
        col_f = lax.broadcasted_iota(jnp.int32, (1, chunk), 1).astype(jnp.float32)

        def head(h, carry):
            base = pl.multiple_of(h * (3 * head_dim), head_dim)
            q = qkv_ref[0, :, pl.ds(base, head_dim)]
            k = qkv_ref[0, :, pl.ds(base + head_dim, head_dim)]
            v = qkv_ref[0, :, pl.ds(base + 2 * head_dim, head_dim)]
            k32[pl.ds(h, chunk, stride=heads_loc), :] = k.astype(jnp.float32)
            v32[pl.ds(h, chunk, stride=heads_loc), :] = v.astype(jnp.float32)
            s = lax.dot_general(q, k, contract_last, preferred_element_type=jnp.float32) * scale
            s = s + slope_ref[h] * col_f
            s = jnp.where(col <= row, s, -1e30)
            m = jnp.max(s, axis=1, keepdims=True)
            p = jnp.exp2(s - m)
            m_s[h] = jnp.broadcast_to(m, (chunk, head_dim))
            l_s[h] = jnp.broadcast_to(jnp.sum(p, axis=1, keepdims=True), (chunk, head_dim))
            acc_s[h] = lax.dot_general(p.astype(jnp.bfloat16), v, contract, preferred_element_type=jnp.float32)
            return carry

        lax.fori_loop(0, heads_loc, head, 0)
        kn_ref[0] = k32[...].astype(jnp.bfloat16)
        vn_ref[0] = v32[...].astype(jnp.bfloat16)

    first = (step - 1) * block

    @pl.when((step > 0) & (first < start))
    def _():
        k32[...] = k_ref[0].astype(jnp.float32)
        v32[...] = v_ref[0].astype(jnp.float32)
        pos_col = first + lax.broadcasted_iota(jnp.int32, (block, head_dim), 0)
        pos = first + lax.broadcasted_iota(jnp.int32, (1, block), 1)
        rel = (pos - start).astype(jnp.float32)

        def head(h, carry):
            base = pl.multiple_of(h * (3 * head_dim), head_dim)
            q = qkv_ref[0, :, pl.ds(base, head_dim)]
            k = k32[pl.ds(h, block, stride=heads_loc), :]
            k = jnp.where(pos_col < start, k, 0.0).astype(jnp.bfloat16)
            v = v32[pl.ds(h, block, stride=heads_loc), :].astype(jnp.bfloat16)
            bias = jnp.where(pos < start, slope_ref[h] * rel, -1e30)
            s = lax.dot_general(q, k, contract_last, preferred_element_type=jnp.float32) * scale + bias
            m_old = m_s[h]
            m_new = jnp.maximum(m_old, jnp.max(s, axis=1, keepdims=True))
            p = jnp.exp2(s - jnp.tile(m_new, (1, block // head_dim)))
            alpha = jnp.exp2(m_old - m_new)
            m_s[h] = m_new
            l_s[h] = l_s[h] * alpha + jnp.sum(p, axis=1, keepdims=True)
            acc_s[h] = acc_s[h] * alpha + lax.dot_general(p.astype(jnp.bfloat16), v, contract, preferred_element_type=jnp.float32)
            return carry

        lax.fori_loop(0, heads_loc, head, 0)

    @pl.when(step == pl.num_programs(1) - 1)
    def _():
        for h in range(heads_loc):
            ctx_ref[0, :, h * head_dim:(h + 1) * head_dim] = (acc_s[h] / l_s[h]).astype(jnp.bfloat16)


def attention(qkv, k_rows, v_rows, prefix_len, slopes, first_seq, heads_loc, head_dim, cache_len):
    seqs, chunk, width = qkv.shape
    block = KV_BLOCK
    blocks = pl.cdiv(cache_len - chunk, block)

    def kv_map(b, j, lens, sl):
        last = jnp.maximum((lens[first_seq + b] + block - 1) // block - 1, 0)
        return (first_seq + b, jnp.clip(j - 1, 0, last), 0)

    kv_spec = pl.BlockSpec((1, block * heads_loc, head_dim), kv_map)
    new_spec = pl.BlockSpec((1, chunk * heads_loc, head_dim), lambda b, j, lens, sl: (b, 0, 0))
    rows_max = max(block, chunk) * heads_loc
    macs = 2 * seqs * chunk * cache_len * heads_loc * head_dim
    return pl.pallas_call(
        functools.partial(attn_kernel, heads_loc, head_dim, block, first_seq),
        grid_spec=pltpu.PrefetchScalarGridSpec(
            num_scalar_prefetch=2,
            grid=(seqs, blocks + 1),
            in_specs=[pl.BlockSpec((1, chunk, width), lambda b, j, lens, sl: (b, 0, 0)), kv_spec, kv_spec],
            out_specs=[pl.BlockSpec((1, chunk, heads_loc * head_dim), lambda b, j, lens, sl: (b, 0, 0)), new_spec, new_spec],
            scratch_shapes=[
                pltpu.VMEM((rows_max, head_dim), jnp.float32),
                pltpu.VMEM((rows_max, head_dim), jnp.float32),
                pltpu.VMEM((heads_loc, chunk, head_dim), jnp.float32),
                pltpu.VMEM((heads_loc, chunk, head_dim), jnp.float32),
                pltpu.VMEM((heads_loc, chunk, head_dim), jnp.float32),
            ],
        ),
        out_shape=[
            jax.ShapeDtypeStruct((seqs, chunk, heads_loc * head_dim), jnp.bfloat16),
            jax.ShapeDtypeStruct((seqs, chunk * heads_loc, head_dim), jnp.bfloat16),
            jax.ShapeDtypeStruct((seqs, chunk * heads_loc, head_dim), jnp.bfloat16),
        ],
        compiler_params=pltpu.CompilerParams(dimension_semantics=("arbitrary", "arbitrary")),
        cost_estimate=pl.CostEstimate(flops=2 * macs, bytes_accessed=4 * seqs * cache_len * heads_loc * head_dim, transcendentals=0),
        name="prefill_attention",
    )(prefix_len, slopes, qkv, k_rows, v_rows)


def solution(mesh):
    tp_size = mesh.shape['tp']

    def local_layer(x_local, prefix_len, k_cache, v_cache, ln1_gain, ln1_bias, w_qkv, b_qkv, w_out, b_out, ln2_gain, ln2_bias, w_up, b_up, w_down, b_down):
        batch_n, tok_loc, d_model = x_local.shape
        cache_len, heads_loc, head_dim = k_cache.shape[1:]
        chunk_len = tok_loc * tp_size
        head_ids = lax.axis_index('tp') * heads_loc + jnp.arange(heads_loc)
        slopes = jnp.exp2(-8.0 * (head_ids + 1).astype(jnp.float32) / (heads_loc * tp_size)) * LOG2E
        k_rows = k_cache.reshape(batch_n, cache_len * heads_loc, head_dim)
        v_rows = v_cache.reshape(batch_n, cache_len * heads_loc, head_dim)
        seqs = batch_n // N_CHUNKS
        core = lax.axis_index('tp') % 2
        pairs = [(i, i ^ 1) for i in range(tp_size)]
        same_core = [[i for i in range(tp_size) if i % 2 == c] for c in range(2)]
        vecs = [v.reshape(1, d_model) for v in (ln1_gain, ln1_bias, b_out, ln2_gain, ln2_bias, b_down)]
        gain1, bias1, bias_out, gain2, bias2, bias_down = vecs

        def gather(rows):
            return lax.all_gather(rows, 'tp', axis=1, tiled=True)

        def reduce_scatter(acts, weights, held=None):
            if not PAIR_FIRST:
                part = jnp.einsum('bce,ed->bcd', acts, weights, preferred_element_type=jnp.float32).astype(jnp.bfloat16)
                return lax.psum_scatter(part, 'tp', scatter_dimension=1, tiled=True)
            by_core = acts.reshape(acts.shape[0], tp_size // 2, 2, tok_loc, acts.shape[-1])

            def half(which):
                mine = lax.dynamic_index_in_dim(by_core, which, axis=2, keepdims=False).reshape(acts.shape[0], chunk_len // 2, acts.shape[-1])
                return jnp.einsum('bce,ed->bcd', mine, weights, preferred_element_type=jnp.float32)

            other = lax.ppermute(half(1 - core).astype(jnp.bfloat16), 'tp', pairs)
            part = (half(core) + other.astype(jnp.float32)).astype(jnp.bfloat16)
            if held is not None:
                part, held[0] = lax.optimization_barrier((part, held[0]))
            return lax.psum_scatter(part, 'tp', scatter_dimension=1, tiled=True, axis_index_groups=same_core)

        normed = [norm_chunk(x_local, gain1, bias1, c * seqs, seqs) for c in range(N_CHUNKS)]
        k_upd, v_upd = (rows.reshape(k_cache.shape) for rows in copy_caches(k_rows, v_rows, normed[-1]))
        gathered = [gather(rows) for rows in normed]
        contexts, writes = [], []
        for c in range(N_CHUNKS):
            qkv = (jnp.einsum('bcd,de->bce', gathered[c], w_qkv, preferred_element_type=jnp.float32) + b_qkv.astype(jnp.float32)).astype(jnp.bfloat16)
            context, k_new, v_new = attention(qkv, k_rows, v_rows, prefix_len, slopes, c * seqs, heads_loc, head_dim, cache_len)
            contexts.append(context)
            k_new = k_new.reshape(seqs, chunk_len, heads_loc, head_dim)
            v_new = v_new.reshape(seqs, chunk_len, heads_loc, head_dim)
            for b in range(seqs):
                at = (c * seqs + b, prefix_len[c * seqs + b], 0, 0)
                writes.append((k_new[b:b + 1], v_new[b:b + 1], at))
        residuals, normed2 = [], []
        for c in range(N_CHUNKS):
            attn_sum = reduce_scatter(contexts[c], w_out)
            residual, rows = add_norm_chunk(x_local, attn_sum, bias_out, gain2, bias2, c * seqs, seqs)
            residuals.append(residual)
            normed2.append(rows)
        x_out = None
        per_group = N_CHUNKS // MLP_GROUPS
        groups = [slice(g * per_group, (g + 1) * per_group) for g in range(MLP_GROUPS)]
        residuals = [jnp.concatenate(residuals[members], axis=0) for members in groups]
        later = [gather(jnp.concatenate(normed2[members], axis=0)) for members in groups]
        later[0], k_upd, v_upd = lax.optimization_barrier((later[0], k_upd, v_upd))
        for k_new, v_new, at in writes:
            k_upd = lax.dynamic_update_slice(k_upd, k_new, at)
            v_upd = lax.dynamic_update_slice(v_upd, v_new, at)
        for g in range(MLP_GROUPS):
            rows = later.pop(0)
            up_pre = jnp.einsum('bcd,df->bcf', rows, w_up, preferred_element_type=jnp.float32) + b_up.astype(jnp.float32)
            up_act = jax.nn.gelu(up_pre, approximate=True).astype(jnp.bfloat16)
            x_out = add_chunk(residuals[g], reduce_scatter(up_act, w_down, later if later else None), bias_down, x_out, g * per_group * seqs, batch_n)
        return x_out, k_upd, v_upd

    tok_spec = P('dp', 'tp', None)
    cache_spec = P('dp', None, 'tp', None)
    replicated = P()
    in_specs = (tok_spec, P('dp'), cache_spec, cache_spec, replicated, replicated, P(None, 'tp'), P('tp'), P('tp', None), replicated, replicated, replicated, P(None, 'tp'), P('tp'), P('tp', None), replicated)
    return jax.shard_map(local_layer, mesh=mesh, in_specs=in_specs, out_specs=(tok_spec, cache_spec, cache_spec), check_vma=False)
```
